32 devices in a mesh: grp: 2 (over x), row: 8 (over z, core), col: 2 (over y).
Axes of the slice: x: 2, y: 2, z: 4, core: 2. Of those that a mesh axis runs over, the one named last changes fastest.
Arguments:
- vectors: float32 [64, 128, 512], P('grp', 'row', 'col'), may hold values from -6 to 6
- disorder: float32 [128, 512], P('row', 'col'), may hold values from -1.5 to 1.5
Outputs:
- cheb_prev: float32 [64, 128, 512], P('grp', 'row', 'col')
- cheb_last: float32 [64, 128, 512], P('grp', 'row', 'col')
- moments: float32 [17], replicated
The draws below stay inside these ranges and needn't reach their ends.
All inputs are finite; a program needn't handle non-finite values.
Results may differ from the reference program's by a relative error of at most 0.0001.
Values sent between devices are 32-bit elements; how exact they have to be, the bound alone decides.
No kernel may reach another device: no remote copies, remote signals or barrier semaphores. Data moves between devices by JAX's collectives and lax.ppermute only.
A program may use at most 64 MiB of HBM per device.

```python
import jax
import jax.numpy as jnp
from jax import lax

STEPS = 8
V_ALL = 64
NR = 128
NC = 512


def shard_levels(key, extent, cuts, least, high):
    level, own = 1.0, jax.random.fold_in(key, 6)
    for dim, blocks in cuts:
        steps = jnp.exp(jax.random.uniform(jax.random.fold_in(own, dim), (blocks,), jnp.float32, least / len(cuts), high / len(cuts)))
        level = level * jnp.repeat(steps, extent[dim] // blocks).reshape([-1 if axis == dim else 1 for axis in range(len(extent))])
    return level


def centred(own_key, dims, width, reach, split=(), held_as=jnp.bfloat16):
    result = jax.random.normal(own_key, dims, jnp.float32) * width
    if len(split) > 0:
        result = shard_levels(own_key, dims, split, -0.22, 0.18) * result
    return jnp.clip(result, min=-reach, max=reach).astype(held_as)


def setup_inputs(seed: int = 0) -> dict:
    seeds = jax.random.split(jax.random.key(seed), 3)
    vectors = centred(seeds[0], (V_ALL, NR, NC), 1.0, 6.0, ((0, 2), (1, 8), (2, 2)), jnp.float32)
    disorder = jnp.clip(jax.random.uniform(seeds[1], (NR, NC), jnp.float32, -1.5, 1.5) * shard_levels(seeds[1], (NR, NC), ((0, 8), (1, 2)), -0.4, 0.0), -1.5, 1.5)
    return {"vectors": vectors, "disorder": disorder}


SCALE = 4.6


def hop(field, disorder, even):
    below = jnp.roll(field, -1, 0)
    above = jnp.roll(field, 1, 0)
    left = jnp.roll(field, 1, 1)
    right = jnp.roll(field, -1, 1)
    vertical = jnp.where(even, below, above)
    return (disorder * field - (left + right + vertical)) / SCALE


def reference(vectors, disorder):
    rows = lax.broadcasted_iota(jnp.int32, (NR, NC), 0)
    cols = lax.broadcasted_iota(jnp.int32, (NR, NC), 1)
    even = (rows + cols) % 2 == 0

    def single(vector):
        older = vector
        newer = hop(vector, disorder, even)
        squares = [jnp.sum(older * older), jnp.sum(newer * newer)]
        crosses = [jnp.sum(newer * older)]
        for step in range(1, STEPS):
            latest = 2.0 * hop(newer, disorder, even) - older
            squares.append(jnp.sum(latest * latest))
            crosses.append(jnp.sum(latest * newer))
            older, newer = newer, latest
        return older, newer, jnp.stack(squares), jnp.stack(crosses)

    older, newer, squares, crosses = lax.map(single, vectors)
    count = float(V_ALL * NR * NC)
    squares = jnp.sum(squares, axis=0) / count
    crosses = jnp.sum(crosses, axis=0) / count
    first = squares[0]
    second = crosses[0]
    values = [first, second]
    for index in range(1, STEPS + 1):
        values.append(2.0 * squares[index] - first)
        if index < STEPS:
            values.append(2.0 * crosses[index] - second)
    return older, newer, jnp.stack(values).astype(jnp.float32)
```

```python
import functools

import jax
import jax.numpy as jnp
from jax import lax
from jax.experimental import pallas as pl
from jax.experimental.pallas import tpu as pltpu
from jax.sharding import PartitionSpec as P

STEPS = 8
SCALE = 4.6
RIM_R = (STEPS + 1) // 2
RIM_C = STEPS
LANES = 128
AXES = ("grp", "row", "col")

VMEM = pl.BlockSpec(memory_space=pltpu.VMEM)
ANY = pl.BlockSpec(memory_space=pl.ANY)


def pack_kernel(vec, dis, top, mid, bot, sem):
    vecs, rows, _ = vec.shape
    copies = []
    for r in range(rows):
        if r < RIM_R:
            dst = top.at[pl.ds(r * vecs, vecs), :]
        elif r < rows - RIM_R:
            dst = mid.at[pl.ds((r - RIM_R) * vecs, vecs), :]
        else:
            dst = bot.at[pl.ds((r - rows + RIM_R) * vecs, vecs), :]
        copies.append(pltpu.make_async_copy(vec.at[:, r, :], dst, sem.at[r]))
    for copy in copies:
        copy.start()
    top[RIM_R * vecs :, :] = dis[:8, :]
    bot[RIM_R * vecs :, :] = dis[rows - 8 :, :]
    for copy in copies:
        copy.wait()


def row_source(p, rows, vecs, lo, top, mid, bot, hi):
    for ref, count in ((lo, RIM_R), (top, RIM_R), (mid, rows - 2 * RIM_R), (bot, RIM_R), (hi, RIM_R)):
        if p < count:
            return ref, p * vecs
        p -= count


def turn_kernel(rows, vecs, lo, top, mid, bot, hi, dis, field, edges, dis_pad):
    groups = LANES // vecs
    padded = rows + 2 * RIM_R
    depth = padded // groups
    cols = dis.shape[1]
    at = RIM_R * vecs
    dis_pad[...] = jnp.concatenate(
        [lo[at + 8 - RIM_R : at + 8, :], dis[...], hi[at : at + RIM_R, :]], axis=0
    )
    for m in range(depth):
        for c in range(0, cols, LANES):
            parts = []
            for g in range(groups):
                ref, line = row_source(g * depth + m, rows, vecs, lo, top, mid, bot, hi)
                parts.append(ref[line : line + vecs, c : c + LANES])
            turned = jnp.concatenate(parts, axis=0).T
            field[m, c : c + LANES, :] = turned
            if c == 0:
                edges[0, m * RIM_C : (m + 1) * RIM_C, :] = turned[:RIM_C]
            if c == cols - LANES:
                edges[1, m * RIM_C : (m + 1) * RIM_C, :] = turned[LANES - RIM_C :]
    at = depth * RIM_C
    edges[0, at : at + padded, :] = dis_pad[:, :LANES]
    edges[1, at : at + padded, :] = dis_pad[:, cols - LANES :]


def energy_kernel(vecs, dis_pad, out):
    padded, cols = dis_pad.shape
    groups = LANES // vecs
    depth = padded // groups
    for m in range(depth):
        for c in range(0, cols, LANES):
            parts = [
                jnp.broadcast_to(dis_pad[g * depth + m : g * depth + m + 1, c : c + LANES], (vecs, LANES))
                for g in range(groups)
            ]
            out[m, c : c + LANES, :] = (jnp.concatenate(parts, axis=0) * (2.0 / SCALE)).T


def step_kernel(rows, vecs, field, energy, left, right, last, stats, buf, ene, acc_ref):
    depth, cols, _ = field.shape
    padded = rows + 2 * RIM_R
    groups = LANES // vecs
    lead = 8 + RIM_C
    at = depth * RIM_C
    for m in range(depth):
        buf[0, m, 8:lead, :] = left[m * RIM_C : (m + 1) * RIM_C, :]
        buf[0, m, lead : lead + cols, :] = field[m]
        buf[0, m, lead + cols : lead + cols + RIM_C, :] = right[m * RIM_C : (m + 1) * RIM_C, :]
        for side, ref, first in ((0, left, LANES - RIM_C), (1, right, 0)):
            parts = [
                jnp.broadcast_to(ref[at + g * depth + m : at + g * depth + m + 1, :], (vecs, LANES))
                for g in range(groups)
            ]
            turned = (jnp.concatenate(parts, axis=0) * (2.0 / SCALE)).T
            ene[side, m] = turned[first : first + RIM_C]
    odd = lax.broadcasted_iota(jnp.int32, (8, LANES), 0) % 2 == 1
    group = lax.broadcasted_iota(jnp.int32, (8, LANES), 1) // vecs
    tiles = (cols + 2 * RIM_C) // 8
    zero = jnp.zeros((8, LANES), jnp.float32)

    def own(parts):
        total = zero
        for m in range(depth):
            place = group * depth + m
            kept = (place >= RIM_R) & (place < RIM_R + rows)
            total = total + jnp.where(kept, parts[m], 0.0)
        return total

    def advance(now, then, first):
        squares, crosses, start = [zero] * depth, [zero] * depth, [zero] * depth
        for t in range(tiles):
            c = 8 + 8 * t
            mine = 0 < t < tiles - 1
            here = [buf[now, m, c : c + 8, :] for m in range(depth)]
            over = pltpu.roll(here[depth - 1], vecs, 1)
            under = pltpu.roll(here[0], LANES - vecs, 1)
            for m in range(depth):
                above = here[m - 1] if m > 0 else over
                below = here[m + 1] if m < depth - 1 else under
                vertical = jnp.where(odd, below, above) if m % 2 else jnp.where(odd, above, below)
                near = buf[now, m, c - 1 : c + 7, :] + buf[now, m, c + 1 : c + 9, :] + vertical
                if mine:
                    e = energy[m, c - lead : c - lead + 8, :]
                else:
                    e = ene[0 if t == 0 else 1, m]
                latest = e * here[m] - (2.0 / SCALE) * near
                if first:
                    latest = 0.5 * latest
                else:
                    latest = latest - buf[then, m, c : c + 8, :]
                buf[then, m, c : c + 8, :] = latest
                if mine:
                    squares[m] = squares[m] + latest * latest
                    crosses[m] = crosses[m] + latest * here[m]
                    if first:
                        start[m] = start[m] + here[m] * here[m]
        return squares, crosses, start

    squares, crosses, start = advance(0, 1, True)
    acc_ref[0] = own(start)
    acc_ref[1] = own(crosses)
    acc_ref[2] = own(squares)

    def body(n, _):
        now = lax.rem(n, 2)
        squares, crosses, _ = advance(now, 1 - now, False)
        acc_ref[2 * n + 1] = own(crosses)
        acc_ref[2 * n + 2] = own(squares)
        return 0

    lax.fori_loop(1, STEPS, body, 0)
    lane = lax.broadcasted_iota(jnp.int32, (8, LANES), 1)
    total = zero
    for k in range(2 * STEPS + 1):
        total = total + jnp.where(lane == k, jnp.sum(acc_ref[k], axis=1, keepdims=True), 0.0)
    stats[...] = jnp.broadcast_to(jnp.sum(total, axis=0, keepdims=True), (8, LANES))
    for m in range(depth):
        last[0, m] = buf[(STEPS - 1) % 2, m, lead : lead + cols, :]
        last[1, m] = buf[STEPS % 2, m, lead : lead + cols, :]


def unturn_kernel(rows, vecs, last, prev_out, last_out, flat, sem):
    depth, cols = last.shape[1:3]
    groups = LANES // vecs
    copies = []
    for k, out in ((0, prev_out), (1, last_out)):
        for m in range(depth):
            for c in range(0, cols, LANES):
                turned = last[k, m, c : c + LANES, :].T
                for g in range(groups):
                    r = g * depth + m - RIM_R
                    if 0 <= r < rows:
                        flat[k, r, :, c : c + LANES] = turned[g * vecs : (g + 1) * vecs]
            for g in range(groups):
                r = g * depth + m - RIM_R
                if 0 <= r < rows:
                    copy = pltpu.make_async_copy(flat.at[k, r], out.at[:, r, :], sem.at[k, r])
                    copy.start()
                    copies.append(copy)
    for copy in copies:
        copy.wait()


def shift(array, axis, by):
    count = lax.axis_size(axis)
    return lax.ppermute(array, axis, [(i, (i + by) % count) for i in range(count)])


def body(vectors, disorder):
    vecs, rows, cols = vectors.shape
    f32 = jnp.float32
    groups = LANES // vecs
    padded = rows + 2 * RIM_R
    depth = padded // groups
    assert vecs * groups == LANES and depth * groups == padded and depth % 2 == 0
    assert rows % 8 == 0 and rows > 2 * RIM_R and cols % LANES == 0
    rim = jax.ShapeDtypeStruct((RIM_R * vecs + 8, cols), f32)
    mid = jax.ShapeDtypeStruct(((rows - 2 * RIM_R) * vecs, cols), f32)
    top, mid, bot = pl.pallas_call(
        pack_kernel,
        out_shape=(rim, mid, rim),
        in_specs=[ANY, VMEM],
        out_specs=(VMEM, VMEM, VMEM),
        scratch_shapes=[pltpu.SemaphoreType.DMA((rows,))],
        name="pack",
    )(vectors, disorder)
    lo = shift(bot, "row", 1)
    hi = shift(top, "row", -1)
    field, edges, dis_pad = pl.pallas_call(
        functools.partial(turn_kernel, rows, vecs),
        out_shape=(
            jax.ShapeDtypeStruct((depth, cols, LANES), f32),
            jax.ShapeDtypeStruct((2, depth * RIM_C + padded, LANES), f32),
            jax.ShapeDtypeStruct((padded, cols), f32),
        ),
        in_specs=[VMEM] * 6,
        out_specs=(VMEM,) * 3,
        name="turn",
    )(lo, top, mid, bot, hi, disorder)
    if lax.axis_size("col") == 2:
        other = shift(edges, "col", 1)
        left, right = other[1], other[0]
    else:
        left, right = shift(edges[1], "col", 1), shift(edges[0], "col", -1)
    energy = pl.pallas_call(
        functools.partial(energy_kernel, vecs),
        out_shape=jax.ShapeDtypeStruct((depth, cols, LANES), f32),
        in_specs=[VMEM],
        out_specs=VMEM,
        name="energy",
    )(dis_pad)
    wide = cols + 2 * RIM_C + 16
    last, stats = pl.pallas_call(
        functools.partial(step_kernel, rows, vecs),
        out_shape=(
            jax.ShapeDtypeStruct((2, depth, cols, LANES), f32),
            jax.ShapeDtypeStruct((8, LANES), f32),
        ),
        in_specs=[VMEM] * 4,
        out_specs=(VMEM, VMEM),
        scratch_shapes=[
            pltpu.VMEM((2, depth, wide, LANES), f32),
            pltpu.VMEM((2, depth, RIM_C, LANES), f32),
            pltpu.VMEM((2 * STEPS + 1, 8, LANES), f32),
        ],
        name="steps",
    )(field, energy, left, right)
    older, newer = pl.pallas_call(
        functools.partial(unturn_kernel, rows, vecs),
        out_shape=(jax.ShapeDtypeStruct(vectors.shape, f32),) * 2,
        in_specs=[VMEM],
        out_specs=(ANY, ANY),
        scratch_shapes=[
            pltpu.VMEM((2, rows, vecs, cols), f32),
            pltpu.SemaphoreType.DMA((2, rows)),
        ],
        name="unturn",
    )(last)
    for axis in ("row", "col", "grp"):
        count, reach = lax.axis_size(axis), 1
        assert count & (count - 1) == 0
        while reach < count:
            stats = stats + lax.ppermute(stats, axis, [(i, i ^ reach) for i in range(count)])
            reach *= 2
    sites = vecs * rows * cols
    for axis in AXES:
        sites *= lax.axis_size(axis)
    sums = stats[0, : 2 * STEPS + 1] / float(sites)
    index = jnp.arange(2 * STEPS + 1)
    base = jnp.where(index % 2 == 0, sums[0], sums[1])
    moments = jnp.where(index < 2, sums, 2.0 * sums - base)
    return older, newer, moments


def solution(mesh):
    return jax.shard_map(
        body,
        mesh=mesh,
        in_specs=(P("grp", "row", "col"), P("row", "col")),
        out_specs=(P("grp", "row", "col"), P("grp", "row", "col"), P()),
        check_vma=False,
    )
```

```python
import functools

import jax
import jax.numpy as jnp
from jax import lax
from jax.experimental import pallas as pl
from jax.experimental.pallas import tpu as pltpu
from jax.sharding import PartitionSpec as P

STEPS = 8
SCALE = 4.6
RIM_R = (STEPS + 1) // 2
RIM_C = STEPS
LANES = 128
AXES = ("grp", "row", "col")
SUMS = 2 * STEPS + 1

VMEM = pl.BlockSpec(memory_space=pltpu.VMEM)
HBM = pl.BlockSpec(memory_space=pltpu.HBM)
F32 = jnp.float32


def pack_kernel(vec, dis, top, bot, vec_out, dis_out, sem):
    vecs, rows, _ = vec.shape
    parts = 4
    some = vecs // parts
    copies = [pltpu.make_async_copy(dis, dis_out, sem.at[parts])]
    for k in range(parts):
        here = pl.ds(k * some, some)
        copies.append(pltpu.make_async_copy(vec.at[here], vec_out.at[here], sem.at[k]))
    for copy in copies:
        copy.start()
    copies[0].wait()
    top[RIM_R * vecs :, :] = dis_out[:8, :]
    bot[RIM_R * vecs :, :] = dis_out[rows - 8 :, :]
    for k in range(parts):
        copies[1 + k].wait()
        for r in range(RIM_R):
            line = r * vecs + k * some
            top[line : line + some, :] = vec_out[k * some : (k + 1) * some, r, :]
            bot[line : line + some, :] = vec_out[k * some : (k + 1) * some, rows - RIM_R + r, :]


def turn_kernel(lo, hi, vec, dis, field, edges, dis_turned):
    vecs, rows, cols = vec.shape
    groups = LANES // vecs
    padded = rows + 2 * RIM_R
    depth = padded // groups
    at = RIM_R * vecs

    def lines(p, c):
        if p < RIM_R:
            return lo[p * vecs : (p + 1) * vecs, c : c + LANES]
        if p < RIM_R + rows:
            return vec[:, p - RIM_R, c : c + LANES]
        p -= RIM_R + rows
        return hi[p * vecs : (p + 1) * vecs, c : c + LANES]

    ends = ((0, 0), (cols - LANES, LANES - RIM_C))
    for c in range(0, cols, LANES):
        for m in range(depth):
            turned = jnp.concatenate([lines(g * depth + m, c) for g in range(groups)], axis=0).T
            field[m, 8 + c : 8 + c + LANES, :] = turned
            for side, (place, first) in enumerate(ends):
                if c == place:
                    edges[side, m * RIM_C : (m + 1) * RIM_C, :] = turned[first : first + RIM_C]
        block = [
            lo[at + 8 - RIM_R : at + 8, c : c + LANES],
            dis[:, c : c + LANES],
            hi[at : at + RIM_R, c : c + LANES],
            jnp.zeros((LANES - padded, LANES), F32),
        ]
        turned = jnp.concatenate(block, axis=0).T * (2.0 / SCALE)
        dis_turned[c : c + LANES, :] = turned
        for side, (place, first) in enumerate(ends):
            if c == place:
                edges[side, depth * RIM_C :, :] = turned[first : first + RIM_C]


def spread_rows(tile, m, vecs, depth):
    index = lax.broadcasted_iota(jnp.int32, (8, LANES), 1) // vecs * depth + m
    return jnp.take_along_axis(tile, index, axis=1)


def advance(depth, vecs, now, then, out, energy, tiles, counted, sums):
    odd = lax.broadcasted_iota(jnp.int32, (8, LANES), 0) % 2 == 1
    for t in tiles:
        here = [now(m, t, 0) for m in range(depth)]
        over = pltpu.roll(here[depth - 1], vecs, 1)
        under = pltpu.roll(here[0], LANES - vecs, 1)
        for m in range(depth):
            above = here[m - 1] if m > 0 else over
            below = here[m + 1] if m < depth - 1 else under
            vertical = jnp.where(odd, below, above) if m % 2 else jnp.where(odd, above, below)
            near = (now(m, t, -1) + now(m, t, 1)) + vertical
            latest = energy(m, t) * here[m] - (2.0 / SCALE) * near
            latest = 0.5 * latest if then is None else latest - then(m, t, 0)
            out(m, t, latest)
            if t in counted:
                sums["s"][m] = sums["s"][m] + latest * latest
                sums["r"][m] = sums["r"][m] + latest * here[m]
                if then is None:
                    sums["0"][m] = sums["0"][m] + here[m] * here[m]


def fresh(depth):
    zero = jnp.zeros((8, LANES), F32)
    return {name: [zero] * depth for name in "sr0"}


def own(parts, rows, vecs):
    depth = len(parts)
    group = lax.broadcasted_iota(jnp.int32, (8, LANES), 1) // vecs
    total = jnp.zeros((8, LANES), F32)
    for m in range(depth):
        place = group * depth + m
        kept = (place >= RIM_R) & (place < RIM_R + rows)
        total = total + jnp.where(kept, parts[m], 0.0)
    return total


def chain(field, odd, even):
    result = [(field, None, odd), (odd, field, even)]
    for n in range(2, STEPS):
        now, other = (odd, even) if n % 2 else (even, odd)
        result.append((now, other, other))
    return result


def inner_kernel(rows, vecs, cols, field, dis_turned, odd, even, partial, ene):
    depth = field.shape[0]
    tiles = cols // 8
    for t in range(tiles):
        tile = dis_turned[8 * t : 8 * t + 8, :]
        for m in range(depth):
            ene[m, 8 * t : 8 * t + 8, :] = spread_rows(tile, m, vecs, depth)

    def reader(ref):
        return lambda m, t, by: ref[m, 8 + 8 * t + by : 16 + 8 * t + by, :]

    def writer(ref):
        def write(m, t, value):
            ref[m, 8 + 8 * t : 16 + 8 * t, :] = value

        return write

    for n, (now, then, out) in enumerate(chain(field, odd, even)):
        sums = fresh(depth)
        advance(
            depth,
            vecs,
            reader(now),
            None if then is None else reader(then),
            writer(out),
            lambda m, t: ene[m, 8 * t : 8 * t + 8, :],
            range(tiles),
            range(1, tiles - 1),
            sums,
        )
        if n == 0:
            partial[0] = own(sums["0"], rows, vecs)
        partial[2 * n + 1] = own(sums["r"], rows, vecs)
        partial[2 * n + 2] = own(sums["s"], rows, vecs)


def edge_kernel(
    rows, vecs, cols, places, sites, field, dis_turned, left, right, partial, ends, spread, start, odd, even, ene
):
    depth = field.shape[0]
    at = depth * RIM_C
    for side, rim, rim_at, mine in ((0, left, 0, (0, 1)), (1, right, 2, (cols // 8 - 2, cols // 8 - 1))):
        order = [None, *mine] if rim_at == 0 else [*mine, None]
        for k, t in enumerate(order):
            if t is None:
                tile = rim[places[side], at : at + 8, :]
            else:
                tile = dis_turned[8 * t : 8 * t + 8, :]
            for m in range(depth):
                if t is None:
                    value = rim[places[side], m * RIM_C : (m + 1) * RIM_C, :]
                else:
                    value = field[m, 8 + 8 * t : 16 + 8 * t, :]
                start[side, m, 8 + 8 * k : 16 + 8 * k, :] = value
                ene[side, m, 8 * k : 8 * k + 8, :] = spread_rows(tile, m, vecs, depth)

    def reader(ref):
        return lambda m, t, by: ref[t[0], m, 8 + 8 * t[1] + by : 16 + 8 * t[1] + by, :]

    def writer(ref):
        def write(m, t, value):
            ref[t[0], m, 8 + 8 * t[1] : 16 + 8 * t[1], :] = value

        return write

    middle = ((0, 1), (1, 1))
    every = [(side, k) for side in (0, 1) for k in (0, 1, 2)]
    lane = lax.broadcasted_iota(jnp.int32, (8, LANES), 1)
    total = jnp.zeros((8, LANES), F32)
    first = []

    def place(total, k, parts):
        value = jnp.sum(partial[k] + own(parts, rows, vecs), axis=1, keepdims=True)
        if k < 2:
            first.append(jnp.sum(value, axis=0, keepdims=True))
        return total + jnp.where(lane == k, value, 0.0)

    for n, (now, then, out) in enumerate(chain(start, odd, even)):
        sums = fresh(depth)
        advance(
            depth,
            vecs,
            reader(now),
            None if then is None else reader(then),
            writer(out),
            lambda m, t: ene[t[0], m, 8 * t[1] : 8 * t[1] + 8, :],
            every if n < STEPS - 1 else middle,
            middle,
            sums,
        )
        if n == 0:
            total = place(total, 0, sums["0"])
        total = place(total, 2 * n + 1, sums["r"]) if n < STEPS else total
        total = place(total, 2 * n + 2, sums["s"])
    line = lane[:1]
    values = jnp.sum(total, axis=0, keepdims=True)
    base = jnp.where(line % 2 == 0, first[0], first[1])
    values = jnp.where(line < 2, values, 2.0 * values - base) * (1.0 / sites)
    spread[...] = jnp.broadcast_to(values[None], spread.shape)
    for k, ref in ((0, odd if STEPS % 2 == 0 else even), (1, even if STEPS % 2 == 0 else odd)):
        for side in (0, 1):
            for m in range(depth):
                ends[k, side, m] = ref[side, m, 16:24, :]


def unturn_kernel(rows, vecs, cols, prev, last, ends, prev_out, last_out, flat, sem):
    depth = prev.shape[0]
    groups = LANES // vecs
    copies = []
    for k, (ref, out) in enumerate(((prev, prev_out), (last, last_out))):
        for m in range(depth):
            for c in range(0, cols, LANES):
                low, high = 8 + c, 8 + c + LANES
                block = []
                if c == 0:
                    block.append(ends[k, 0, m])
                    low += 8
                if c == cols - LANES:
                    high -= 8
                block.append(ref[m, low:high, :])
                if c == cols - LANES:
                    block.append(ends[k, 1, m])
                turned = jnp.concatenate(block, axis=0).T
                for g in range(groups):
                    r = g * depth + m - RIM_R
                    if 0 <= r < rows:
                        flat[k, r, :, c : c + LANES] = turned[g * vecs : (g + 1) * vecs]
            for g in range(groups):
                r = g * depth + m - RIM_R
                if 0 <= r < rows:
                    copy = pltpu.make_async_copy(flat.at[k, r], out.at[:, r, :], sem.at[k, r])
                    copy.start()
                    copies.append(copy)
    for copy in copies:
        copy.wait()


def shift(array, axis, by):
    count = lax.axis_size(axis)
    return lax.ppermute(array, axis, [(i, (i + by) % count) for i in range(count)])


def shape(*dims):
    return jax.ShapeDtypeStruct(dims, F32)


def call(kernel, name, limit, ins, outs, scratch, args, out_specs=None):
    return pl.pallas_call(
        kernel,
        out_shape=outs,
        in_specs=ins,
        out_specs=(VMEM,) * len(outs) if out_specs is None else out_specs,
        scratch_shapes=scratch,
        compiler_params=pltpu.CompilerParams(vmem_limit_bytes=limit << 20),
        name=name,
    )(*args)


def body(vectors, disorder):
    vecs, rows, cols = vectors.shape
    groups = LANES // vecs
    padded = rows + 2 * RIM_R
    depth = padded // groups
    assert vecs * groups == LANES and depth * groups == padded and depth % 2 == 0
    assert rows % 8 == 0 and rows >= 2 * RIM_R and cols % LANES == 0 and cols > 2 * RIM_C
    sites, world = vecs * rows * cols, 1
    for axis in AXES:
        sites *= lax.axis_size(axis)
        world *= lax.axis_size(axis)
    dma = pltpu.SemaphoreType.DMA

    rim = shape(RIM_R * vecs + 8, cols)
    top, bot, vec, dis = call(
        pack_kernel,
        "pack",
        4,
        [HBM, HBM],
        (rim, rim, shape(*vectors.shape), shape(*disorder.shape)),
        [dma((5,))],
        (vectors, disorder),
    )
    lo = shift(bot, "row", 1)
    hi = shift(top, "row", -1)
    wide = cols + 16
    wide += (8 - wide) % 32
    tall = shape(depth, wide, LANES)
    field, edges, dis_turned = call(
        turn_kernel,
        "turn",
        6,
        [VMEM] * 4,
        (tall, shape(2, depth * RIM_C + 8, LANES), shape(cols, LANES)),
        [],
        (lo, hi, vec, dis),
    )
    if lax.axis_size("col") == 2:
        left = right = shift(edges, "col", 1)
        places = (1, 0)
    else:
        left, right = shift(edges[1:], "col", 1), shift(edges[:1], "col", -1)
        places = (0, 0)
    odd, even, partial = call(
        functools.partial(inner_kernel, rows, vecs, cols),
        "inner",
        8,
        [VMEM] * 2,
        (tall, tall, shape(SUMS, 8, LANES)),
        [pltpu.VMEM((depth, cols + 8, LANES), F32)],
        (field, dis_turned),
    )
    strip = pltpu.VMEM((2, depth, 40, LANES), F32)
    ends, spread = call(
        functools.partial(edge_kernel, rows, vecs, cols, places, float(sites)),
        "edge",
        6,
        [VMEM] * 5,
        (shape(2, 2, depth, 8, LANES), shape(world, 1, LANES)),
        [strip, strip, strip, pltpu.VMEM((2, depth, 24, LANES), F32)],
        (field, dis_turned, left, right, partial),
    )
    older, newer = call(
        functools.partial(unturn_kernel, rows, vecs, cols),
        "unturn",
        6,
        [VMEM] * 3,
        (shape(*vectors.shape),) * 2,
        [pltpu.VMEM((2, rows, vecs, cols), F32), dma((2, rows))],
        ((odd, even) if STEPS % 2 == 0 else (even, odd)) + (ends,),
        (HBM, HBM),
    )
    moments = jnp.sum(lax.all_to_all(spread, AXES, 0, 0), axis=0)[0, :SUMS]
    return older, newer, moments


def solution(mesh):
    return jax.shard_map(
        body,
        mesh=mesh,
        in_specs=(P("grp", "row", "col"), P("row", "col")),
        out_specs=(P("grp", "row", "col"), P("grp", "row", "col"), P()),
        check_vma=False,
    )
```

```python
import functools

import jax
import jax.numpy as jnp
from jax import lax
from jax.experimental import pallas as pl
from jax.experimental.pallas import tpu as pltpu
from jax.sharding import PartitionSpec as P

STEPS = 8
SCALE = 4.6
RIM_R = (STEPS + 1) // 2
RIM_C = STEPS
LANES = 128
AXES = ("grp", "row", "col")
SUMS = 2 * STEPS + 1

VMEM = pl.BlockSpec(memory_space=pltpu.VMEM)
HBM = pl.BlockSpec(memory_space=pltpu.HBM)
F32 = jnp.float32


def pack_kernel(vec, dis, top, bot, vec_out, dis_out, sem):
    vecs, rows, _ = vec.shape
    parts = 4
    some = vecs // parts
    copies = [pltpu.make_async_copy(dis, dis_out, sem.at[parts])]
    for k in range(parts):
        here = pl.ds(k * some, some)
        copies.append(pltpu.make_async_copy(vec.at[here], vec_out.at[here], sem.at[k]))
    for copy in copies:
        copy.start()
    copies[0].wait()
    top[RIM_R * vecs :, :] = dis_out[:8, :]
    bot[RIM_R * vecs :, :] = dis_out[rows - 8 :, :]
    for k in range(parts):
        copies[1 + k].wait()
        for r in range(RIM_R):
            line = r * vecs + k * some
            top[line : line + some, :] = vec_out[k * some : (k + 1) * some, r, :]
            bot[line : line + some, :] = vec_out[k * some : (k + 1) * some, rows - RIM_R + r, :]


def turn_kernel(lo, hi, vec, dis, field, edges, dis_turned):
    vecs, rows, cols = vec.shape
    groups = LANES // vecs
    padded = rows + 2 * RIM_R
    depth = padded // groups
    at = RIM_R * vecs

    def lines(p, c):
        if p < RIM_R:
            return lo[p * vecs : (p + 1) * vecs, c : c + LANES]
        if p < RIM_R + rows:
            return vec[:, p - RIM_R, c : c + LANES]
        p -= RIM_R + rows
        return hi[p * vecs : (p + 1) * vecs, c : c + LANES]

    ends = ((0, 0), (cols - LANES, LANES - RIM_C))
    for c in range(0, cols, LANES):
        for m in range(depth):
            turned = jnp.concatenate([lines(g * depth + m, c) for g in range(groups)], axis=0).T
            field[m, 8 + c : 8 + c + LANES, :] = turned
            for side, (place, first) in enumerate(ends):
                if c == place:
                    edges[side, m * RIM_C : (m + 1) * RIM_C, :] = turned[first : first + RIM_C]
        block = [
            lo[at + 8 - RIM_R : at + 8, c : c + LANES],
            dis[:, c : c + LANES],
            hi[at : at + RIM_R, c : c + LANES],
            jnp.zeros((LANES - padded, LANES), F32),
        ]
        turned = jnp.concatenate(block, axis=0).T * (2.0 / SCALE)
        dis_turned[c : c + LANES, :] = turned
        for side, (place, first) in enumerate(ends):
            if c == place:
                edges[side, depth * RIM_C :, :] = turned[first : first + RIM_C]


def spread_rows(tile, m, vecs, depth):
    index = lax.broadcasted_iota(jnp.int32, (8, LANES), 1) // vecs * depth + m
    return jnp.take_along_axis(tile, index, axis=1)


def advance(depth, vecs, now, then, out, energy, tiles, counted, sums):
    odd = lax.broadcasted_iota(jnp.int32, (8, LANES), 0) % 2 == 1
    for t in tiles:
        here = [now(m, t, 0) for m in range(depth)]
        over = pltpu.roll(here[depth - 1], vecs, 1)
        under = pltpu.roll(here[0], LANES - vecs, 1)
        for m in range(depth):
            above = here[m - 1] if m > 0 else over
            below = here[m + 1] if m < depth - 1 else under
            vertical = jnp.where(odd, below, above) if m % 2 else jnp.where(odd, above, below)
            near = (now(m, t, -1) + now(m, t, 1)) + vertical
            latest = energy(m, t) * here[m] - (2.0 / SCALE) * near
            latest = 0.5 * latest if then is None else latest - then(m, t, 0)
            out(m, t, latest)
            if t in counted:
                sums["s"][m] = sums["s"][m] + latest * latest
                sums["r"][m] = sums["r"][m] + latest * here[m]
                if then is None:
                    sums["0"][m] = sums["0"][m] + here[m] * here[m]


def fresh(depth):
    zero = jnp.zeros((8, LANES), F32)
    return {name: [zero] * depth for name in "sr0"}


def own(parts, rows, vecs):
    depth = len(parts)
    group = lax.broadcasted_iota(jnp.int32, (8, LANES), 1) // vecs
    total = jnp.zeros((8, LANES), F32)
    for m in range(depth):
        place = group * depth + m
        kept = (place >= RIM_R) & (place < RIM_R + rows)
        total = total + jnp.where(kept, parts[m], 0.0)
    return total


def chain(field, odd, even):
    result = [(field, None, odd), (odd, field, even)]
    for n in range(2, STEPS):
        now, other = (odd, even) if n % 2 else (even, odd)
        result.append((now, other, other))
    return result


def inner_kernel(rows, vecs, cols, field, dis_turned, odd, even, partial, ene):
    depth = field.shape[0]
    tiles = cols // 8
    for t in range(tiles):
        tile = dis_turned[8 * t : 8 * t + 8, :]
        for m in range(depth):
            ene[m, 8 * t : 8 * t + 8, :] = spread_rows(tile, m, vecs, depth)

    def reader(ref):
        return lambda m, t, by: ref[m, 8 + 8 * t + by : 16 + 8 * t + by, :]

    def writer(ref):
        def write(m, t, value):
            ref[m, 8 + 8 * t : 16 + 8 * t, :] = value

        return write

    for n, (now, then, out) in enumerate(chain(field, odd, even)):
        sums = fresh(depth)
        advance(
            depth,
            vecs,
            reader(now),
            None if then is None else reader(then),
            writer(out),
            lambda m, t: ene[m, 8 * t : 8 * t + 8, :],
            range(tiles),
            range(1, tiles - 1),
            sums,
        )
        if n == 0:
            partial[0] = own(sums["0"], rows, vecs)
        partial[2 * n + 1] = own(sums["r"], rows, vecs)
        partial[2 * n + 2] = own(sums["s"], rows, vecs)


def edge_kernel(
    rows, vecs, cols, places, sites, field, dis_turned, left, right, partial, ends, spread, start, odd, even, ene
):
    depth = field.shape[0]
    at = depth * RIM_C
    for side, rim, rim_at, mine in ((0, left, 0, (0, 1)), (1, right, 2, (cols // 8 - 2, cols // 8 - 1))):
        order = [None, *mine] if rim_at == 0 else [*mine, None]
        for k, t in enumerate(order):
            if t is None:
                tile = rim[places[side], at : at + 8, :]
            else:
                tile = dis_turned[8 * t : 8 * t + 8, :]
            for m in range(depth):
                if t is None:
                    value = rim[places[side], m * RIM_C : (m + 1) * RIM_C, :]
                else:
                    value = field[m, 8 + 8 * t : 16 + 8 * t, :]
                start[side, m, 8 + 8 * k : 16 + 8 * k, :] = value
                ene[side, m, 8 * k : 8 * k + 8, :] = spread_rows(tile, m, vecs, depth)

    def reader(ref):
        return lambda m, t, by: ref[t[0], m, 8 + 8 * t[1] + by : 16 + 8 * t[1] + by, :]

    def writer(ref):
        def write(m, t, value):
            ref[t[0], m, 8 + 8 * t[1] : 16 + 8 * t[1], :] = value

        return write

    middle = ((0, 1), (1, 1))
    every = [(side, k) for side in (0, 1) for k in (0, 1, 2)]
    lane = lax.broadcasted_iota(jnp.int32, (8, LANES), 1)
    total = jnp.zeros((8, LANES), F32)
    first = []

    def place(total, k, parts):
        value = jnp.sum(partial[k] + own(parts, rows, vecs), axis=1, keepdims=True)
        if k < 2:
            first.append(jnp.sum(value, axis=0, keepdims=True))
        return total + jnp.where(lane == k, value, 0.0)

    for n, (now, then, out) in enumerate(chain(start, odd, even)):
        sums = fresh(depth)
        advance(
            depth,
            vecs,
            reader(now),
            None if then is None else reader(then),
            writer(out),
            lambda m, t: ene[t[0], m, 8 * t[1] : 8 * t[1] + 8, :],
            every if n < STEPS - 1 else middle,
            middle,
            sums,
        )
        if n == 0:
            total = place(total, 0, sums["0"])
        total = place(total, 2 * n + 1, sums["r"]) if n < STEPS else total
        total = place(total, 2 * n + 2, sums["s"])
    line = lane[:1]
    values = jnp.sum(total, axis=0, keepdims=True)
    base = jnp.where(line % 2 == 0, first[0], first[1])
    values = jnp.where(line < 2, values, 2.0 * values - base) * (1.0 / sites)
    spread[...] = jnp.broadcast_to(values[None], spread.shape)
    for k, ref in ((0, odd if STEPS % 2 == 0 else even), (1, even if STEPS % 2 == 0 else odd)):
        for side in (0, 1):
            for m in range(depth):
                ends[k, side, m] = ref[side, m, 16:24, :]


def unturn_kernel(rows, vecs, cols, prev, last, ends, prev_out, last_out, flat, sem):
    depth = prev.shape[0]
    groups = LANES // vecs
    copies = []
    for k, (ref, out) in enumerate(((prev, prev_out), (last, last_out))):
        for m in range(depth):
            for c in range(0, cols, LANES):
                low, high = 8 + c, 8 + c + LANES
                block = []
                if c == 0:
                    block.append(ends[k, 0, m])
                    low += 8
                if c == cols - LANES:
                    high -= 8
                block.append(ref[m, low:high, :])
                if c == cols - LANES:
                    block.append(ends[k, 1, m])
                turned = jnp.concatenate(block, axis=0).T
                for g in range(groups):
                    r = g * depth + m - RIM_R
                    if 0 <= r < rows:
                        flat[k, r, :, c : c + LANES] = turned[g * vecs : (g + 1) * vecs]
            for g in range(groups):
                r = g * depth + m - RIM_R
                if 0 <= r < rows:
                    copy = pltpu.make_async_copy(flat.at[k, r], out.at[:, r, :], sem.at[k, r])
                    copy.start()
                    copies.append(copy)
    for copy in copies:
        copy.wait()


def shift(array, axis, by):
    count = lax.axis_size(axis)
    return lax.ppermute(array, axis, [(i, (i + by) % count) for i in range(count)])


def shape(*dims):
    return jax.ShapeDtypeStruct(dims, F32)


def call(kernel, name, limit, ins, outs, scratch, args, out_specs=None):
    return pl.pallas_call(
        kernel,
        out_shape=outs,
        in_specs=ins,
        out_specs=(VMEM,) * len(outs) if out_specs is None else out_specs,
        scratch_shapes=scratch,
        compiler_params=pltpu.CompilerParams(vmem_limit_bytes=limit << 20),
        name=name,
    )(*args)


def body(vectors, disorder):
    vecs, rows, cols = vectors.shape
    groups = LANES // vecs
    padded = rows + 2 * RIM_R
    depth = padded // groups
    assert vecs * groups == LANES and depth * groups == padded and depth % 2 == 0
    assert rows % 8 == 0 and rows >= 2 * RIM_R and cols % LANES == 0 and cols > 2 * RIM_C
    sites, world = vecs * rows * cols, 1
    for axis in AXES:
        sites *= lax.axis_size(axis)
        world *= lax.axis_size(axis)
    dma = pltpu.SemaphoreType.DMA

    rim = shape(RIM_R * vecs + 8, cols)
    top, bot, vec, dis = call(
        pack_kernel,
        "pack",
        4,
        [HBM, HBM],
        (rim, rim, shape(*vectors.shape), shape(*disorder.shape)),
        [dma((5,))],
        (
            pltpu.with_memory_space_constraint(vectors, pltpu.HBM),
            pltpu.with_memory_space_constraint(disorder, pltpu.HBM),
        ),
    )
    lo = shift(bot, "row", 1)
    hi = shift(top, "row", -1)
    wide = cols + 16
    wide += (8 - wide) % 32
    tall = shape(depth, wide, LANES)
    field, edges, dis_turned = call(
        turn_kernel,
        "turn",
        6,
        [VMEM] * 4,
        (tall, shape(2, depth * RIM_C + 8, LANES), shape(cols, LANES)),
        [],
        (lo, hi, vec, dis),
    )
    if lax.axis_size("col") == 2:
        left = right = shift(edges, "col", 1)
        places = (1, 0)
    else:
        left, right = shift(edges[1:], "col", 1), shift(edges[:1], "col", -1)
        places = (0, 0)
    odd, even, partial = call(
        functools.partial(inner_kernel, rows, vecs, cols),
        "inner",
        8,
        [VMEM] * 2,
        (tall, tall, shape(SUMS, 8, LANES)),
        [pltpu.VMEM((depth, cols + 8, LANES), F32)],
        (field, dis_turned),
    )
    strip = pltpu.VMEM((2, depth, 40, LANES), F32)
    ends, spread = call(
        functools.partial(edge_kernel, rows, vecs, cols, places, float(sites)),
        "edge",
        6,
        [VMEM] * 5,
        (shape(2, 2, depth, 8, LANES), pltpu.VMEM((world, 1, LANES), F32)),
        [strip, strip, strip, pltpu.VMEM((2, depth, 24, LANES), F32)],
        (field, dis_turned, left, right, partial),
    )
    older, newer = call(
        functools.partial(unturn_kernel, rows, vecs, cols),
        "unturn",
        6,
        [VMEM] * 3,
        (shape(*vectors.shape),) * 2,
        [pltpu.VMEM((2, rows, vecs, cols), F32), dma((2, rows))],
        ((odd, even) if STEPS % 2 == 0 else (even, odd)) + (ends,),
        (HBM, HBM),
    )
    moments = jnp.sum(lax.all_to_all(spread, AXES, 0, 0), axis=0)[0, :SUMS]
    return older, newer, moments


def solution(mesh):
    return jax.shard_map(
        body,
        mesh=mesh,
        in_specs=(P("grp", "row", "col"), P("row", "col")),
        out_specs=(P("grp", "row", "col"), P("grp", "row", "col"), P()),
        check_vma=False,
    )
```

```python
import functools

import jax
import jax.numpy as jnp
from jax import lax
from jax.experimental import pallas as pl
from jax.experimental.pallas import tpu as pltpu
from jax.sharding import PartitionSpec as P

STEPS = 8
SCALE = 4.6
RIM_R = (STEPS + 1) // 2
RIM_C = STEPS
LANES = 128
AXES = ("grp", "row", "col")
SUMS = 2 * STEPS + 1

VMEM = pl.BlockSpec(memory_space=pltpu.VMEM)
HBM = pl.BlockSpec(memory_space=pltpu.HBM)
F32 = jnp.float32


def pack_kernel(vec, dis, top, bot, sem):
    vecs, rows, _ = vec.shape
    copies = []
    for k, (out, first) in enumerate(((top, 0), (bot, rows - RIM_R))):
        place = pl.ds(first, RIM_R)
        copies.append(pltpu.make_async_copy(vec.at[:, place, :], out.at[pl.ds(0, vecs)], sem.at[k, 0]))
        copies.append(pltpu.make_async_copy(dis.at[place, :], out.at[vecs], sem.at[k, 1]))
    for copy in copies:
        copy.start()
    for copy in copies:
        copy.wait()


def load_kernel(after, vec, dis, vec_out, dis_out, sem):
    copies = [
        pltpu.make_async_copy(vec, vec_out, sem.at[0]),
        pltpu.make_async_copy(dis, dis_out, sem.at[1]),
    ]
    for copy in copies:
        copy.start()
    for copy in copies:
        copy.wait()


def turn_kernel(lo, hi, vec, dis, field, edges, dis_turned):
    vecs, rows, cols = vec.shape
    groups = LANES // vecs
    padded = rows + 2 * RIM_R
    depth = padded // groups

    def lines(p, c):
        if p < RIM_R:
            return lo[:vecs, p, c : c + LANES]
        if p < RIM_R + rows:
            return vec[:, p - RIM_R, c : c + LANES]
        return hi[:vecs, p - RIM_R - rows, c : c + LANES]

    ends = ((0, 0), (cols - LANES, LANES - RIM_C))
    for c in range(0, cols, LANES):
        for m in range(depth):
            turned = jnp.concatenate([lines(g * depth + m, c) for g in range(groups)], axis=0).T
            field[m, 8 + c : 8 + c + LANES, :] = turned
            for side, (place, first) in enumerate(ends):
                if c == place:
                    edges[side, m * RIM_C : (m + 1) * RIM_C, :] = turned[first : first + RIM_C]
        block = [
            lo[vecs, :, c : c + LANES],
            dis[:, c : c + LANES],
            hi[vecs, :, c : c + LANES],
            jnp.zeros((LANES - padded, LANES), F32),
        ]
        turned = jnp.concatenate(block, axis=0).T * (2.0 / SCALE)
        dis_turned[c : c + LANES, :] = turned
        for side, (place, first) in enumerate(ends):
            if c == place:
                edges[side, depth * RIM_C :, :] = turned[first : first + RIM_C]


def spread_rows(tile, m, vecs, depth):
    index = lax.broadcasted_iota(jnp.int32, (8, LANES), 1) // vecs * depth + m
    return jnp.take_along_axis(tile, index, axis=1)


def advance(depth, vecs, now, then, out, energy, tiles, counted, sums):
    odd = lax.broadcasted_iota(jnp.int32, (8, LANES), 0) % 2 == 1
    for t in tiles:
        here = [now(m, t, 0) for m in range(depth)]
        over = pltpu.roll(here[depth - 1], vecs, 1)
        under = pltpu.roll(here[0], LANES - vecs, 1)
        for m in range(depth):
            above = here[m - 1] if m > 0 else over
            below = here[m + 1] if m < depth - 1 else under
            vertical = jnp.where(odd, below, above) if m % 2 else jnp.where(odd, above, below)
            near = (now(m, t, -1) + now(m, t, 1)) + vertical
            latest = energy(m, t) * here[m] - (2.0 / SCALE) * near
            latest = 0.5 * latest if then is None else latest - then(m, t, 0)
            out(m, t, latest)
            if t in counted:
                sums["s"][m] = sums["s"][m] + latest * latest
                sums["r"][m] = sums["r"][m] + latest * here[m]
                if then is None:
                    sums["0"][m] = sums["0"][m] + here[m] * here[m]


def fresh(depth):
    zero = jnp.zeros((8, LANES), F32)
    return {name: [zero] * depth for name in "sr0"}


def own(parts, rows, vecs):
    depth = len(parts)
    group = lax.broadcasted_iota(jnp.int32, (8, LANES), 1) // vecs
    total = jnp.zeros((8, LANES), F32)
    for m in range(depth):
        place = group * depth + m
        kept = (place >= RIM_R) & (place < RIM_R + rows)
        total = total + jnp.where(kept, parts[m], 0.0)
    return total


def chain(field, odd, even):
    result = [(field, None, odd), (odd, field, even)]
    for n in range(2, STEPS):
        now, other = (odd, even) if n % 2 else (even, odd)
        result.append((now, other, other))
    return result


def inner_kernel(rows, vecs, cols, field, dis_turned, odd, even, partial, ene):
    depth = field.shape[0]
    tiles = cols // 8
    for t in range(tiles):
        tile = dis_turned[8 * t : 8 * t + 8, :]
        for m in range(depth):
            ene[m, 8 * t : 8 * t + 8, :] = spread_rows(tile, m, vecs, depth)

    def reader(ref):
        return lambda m, t, by: ref[m, 8 + 8 * t + by : 16 + 8 * t + by, :]

    def writer(ref):
        def write(m, t, value):
            ref[m, 8 + 8 * t : 16 + 8 * t, :] = value

        return write

    for n, (now, then, out) in enumerate(chain(field, odd, even)):
        sums = fresh(depth)
        advance(
            depth,
            vecs,
            reader(now),
            None if then is None else reader(then),
            writer(out),
            lambda m, t: ene[m, 8 * t : 8 * t + 8, :],
            range(tiles),
            range(1, tiles - 1),
            sums,
        )
        if n == 0:
            partial[0] = own(sums["0"], rows, vecs)
        partial[2 * n + 1] = own(sums["r"], rows, vecs)
        partial[2 * n + 2] = own(sums["s"], rows, vecs)


def edge_kernel(
    rows, vecs, cols, places, sites, field, dis_turned, left, right, partial, ends, spread, start, odd, even, ene
):
    depth = field.shape[0]
    at = depth * RIM_C
    for side, rim, rim_at, mine in ((0, left, 0, (0, 1)), (1, right, 2, (cols // 8 - 2, cols // 8 - 1))):
        order = [None, *mine] if rim_at == 0 else [*mine, None]
        for k, t in enumerate(order):
            if t is None:
                tile = rim[places[side], at : at + 8, :]
            else:
                tile = dis_turned[8 * t : 8 * t + 8, :]
            for m in range(depth):
                if t is None:
                    value = rim[places[side], m * RIM_C : (m + 1) * RIM_C, :]
                else:
                    value = field[m, 8 + 8 * t : 16 + 8 * t, :]
                start[side, m, 8 + 8 * k : 16 + 8 * k, :] = value
                ene[side, m, 8 * k : 8 * k + 8, :] = spread_rows(tile, m, vecs, depth)

    def reader(ref):
        return lambda m, t, by: ref[t[0], m, 8 + 8 * t[1] + by : 16 + 8 * t[1] + by, :]

    def writer(ref):
        def write(m, t, value):
            ref[t[0], m, 8 + 8 * t[1] : 16 + 8 * t[1], :] = value

        return write

    middle = ((0, 1), (1, 1))
    every = [(side, k) for side in (0, 1) for k in (0, 1, 2)]
    lane = lax.broadcasted_iota(jnp.int32, (8, LANES), 1)
    total = jnp.zeros((8, LANES), F32)
    first = []

    def place(total, k, parts):
        value = jnp.sum(partial[k] + own(parts, rows, vecs), axis=1, keepdims=True)
        if k < 2:
            first.append(jnp.sum(value, axis=0, keepdims=True))
        return total + jnp.where(lane == k, value, 0.0)

    for n, (now, then, out) in enumerate(chain(start, odd, even)):
        sums = fresh(depth)
        advance(
            depth,
            vecs,
            reader(now),
            None if then is None else reader(then),
            writer(out),
            lambda m, t: ene[t[0], m, 8 * t[1] : 8 * t[1] + 8, :],
            every if n < STEPS - 1 else middle,
            middle,
            sums,
        )
        if n == 0:
            total = place(total, 0, sums["0"])
        total = place(total, 2 * n + 1, sums["r"]) if n < STEPS else total
        total = place(total, 2 * n + 2, sums["s"])
    line = lane[:1]
    values = jnp.sum(total, axis=0, keepdims=True)
    base = jnp.where(line % 2 == 0, first[0], first[1])
    values = jnp.where(line < 2, values, 2.0 * values - base) * (1.0 / sites)
    spread[...] = jnp.broadcast_to(values[None], spread.shape)
    for k, ref in ((0, odd if STEPS % 2 == 0 else even), (1, even if STEPS % 2 == 0 else odd)):
        for side in (0, 1):
            for m in range(depth):
                ends[k, side, m] = ref[side, m, 16:24, :]


def on_first_chip():
    return (lax.axis_index("grp") == 0) & (lax.axis_index("row") < 2) & (lax.axis_index("col") == 0)


def unturn(rows, vecs, cols, prev, last, ends, prev_out, last_out, flat, sem):
    depth = prev.shape[0]
    groups = LANES // vecs
    copies = []
    for k, (ref, out) in enumerate(((prev, prev_out), (last, last_out))):
        for m in range(depth):
            for c in range(0, cols, LANES):
                low, high = 8 + c, 8 + c + LANES
                block = []
                if c == 0:
                    block.append(ends[k, 0, m])
                    low += 8
                if c == cols - LANES:
                    high -= 8
                block.append(ref[m, low:high, :])
                if c == cols - LANES:
                    block.append(ends[k, 1, m])
                turned = jnp.concatenate(block, axis=0).T
                for g in range(groups):
                    r = g * depth + m - RIM_R
                    if 0 <= r < rows:
                        flat[k, :, r, c : c + LANES] = turned[g * vecs : (g + 1) * vecs]
        copy = pltpu.make_async_copy(flat.at[k], out, sem.at[k])
        copy.start()
        copies.append(copy)
    for copy in copies:
        copy.wait()


def before_kernel(rows, vecs, cols, prev, last, ends, spread, prev_out, last_out, spread_out, flat, sem):
    spread_out[...] = spread[...]

    @pl.when(on_first_chip())
    def _():
        unturn(rows, vecs, cols, prev, last, ends, prev_out, last_out, flat, sem)


def after_kernel(rows, vecs, cols, sums, prev, last, ends, prev_in, last_in, prev_out, last_out, moments, flat, sem):
    moments[...] = jnp.sum(sums[...], axis=0)[:, :SUMS]

    @pl.when(jnp.logical_not(on_first_chip()))
    def _():
        unturn(rows, vecs, cols, prev, last, ends, prev_out, last_out, flat, sem)


def shift(array, axis, by):
    count = lax.axis_size(axis)
    return lax.ppermute(array, axis, [(i, (i + by) % count) for i in range(count)])


def shape(*dims):
    return jax.ShapeDtypeStruct(dims, F32)


def call(kernel, name, limit, ins, outs, scratch, args, out_specs=None, aliases={}):
    return pl.pallas_call(
        kernel,
        out_shape=outs,
        in_specs=ins,
        out_specs=(VMEM,) * len(outs) if out_specs is None else out_specs,
        scratch_shapes=scratch,
        input_output_aliases=aliases,
        compiler_params=pltpu.CompilerParams(vmem_limit_bytes=limit << 20),
        name=name,
    )(*args)


def body(vectors, disorder):
    vecs, rows, cols = vectors.shape
    groups = LANES // vecs
    padded = rows + 2 * RIM_R
    depth = padded // groups
    assert vecs * groups == LANES and depth * groups == padded and depth % 2 == 0
    assert rows % 8 == 0 and rows >= 2 * RIM_R and cols % LANES == 0 and cols > 2 * RIM_C
    sites, world = vecs * rows * cols, 1
    for axis in AXES:
        sites *= lax.axis_size(axis)
        world *= lax.axis_size(axis)
    dma = pltpu.SemaphoreType.DMA

    rim = shape(vecs + 1, RIM_R, cols)
    inputs = (
        pltpu.with_memory_space_constraint(vectors, pltpu.HBM),
        pltpu.with_memory_space_constraint(disorder, pltpu.HBM),
    )
    top, bot = call(pack_kernel, "pack", 2, [HBM, HBM], (rim, rim), [dma((2, 2))], inputs)
    vec, dis = call(
        load_kernel,
        "load",
        2,
        [VMEM, HBM, HBM],
        (shape(*vectors.shape), shape(*disorder.shape)),
        [dma((2,))],
        (top,) + inputs,
    )
    lo = shift(bot, "row", 1)
    hi = shift(top, "row", -1)
    wide = cols + 16
    wide += (8 - wide) % 32
    tall = shape(depth, wide, LANES)
    field, edges, dis_turned = call(
        turn_kernel,
        "turn",
        6,
        [VMEM] * 4,
        (tall, shape(2, depth * RIM_C + 8, LANES), shape(cols, LANES)),
        [],
        (lo, hi, vec, dis),
    )
    if lax.axis_size("col") == 2:
        left = right = shift(edges, "col", 1)
        places = (1, 0)
    else:
        left, right = shift(edges[1:], "col", 1), shift(edges[:1], "col", -1)
        places = (0, 0)
    odd, even, partial = call(
        functools.partial(inner_kernel, rows, vecs, cols),
        "inner",
        8,
        [VMEM] * 2,
        (tall, tall, shape(SUMS, 8, LANES)),
        [pltpu.VMEM((depth, cols + 8, LANES), F32)],
        (field, dis_turned),
    )
    strip = pltpu.VMEM((2, depth, 40, LANES), F32)
    ends, spread = call(
        functools.partial(edge_kernel, rows, vecs, cols, places, float(sites)),
        "edge",
        6,
        [VMEM] * 5,
        (shape(2, 2, depth, 8, LANES), shape(world, 1, LANES)),
        [strip, strip, strip, pltpu.VMEM((2, depth, 24, LANES), F32)],
        (field, dis_turned, left, right, partial),
    )
    fields = ((odd, even) if STEPS % 2 == 0 else (even, odd)) + (ends,)
    whole = (shape(*vectors.shape),) * 2
    scratch = [pltpu.VMEM((2, vecs, rows, cols), F32), dma((2,))]
    older, newer, spread = call(
        functools.partial(before_kernel, rows, vecs, cols),
        "before",
        6,
        [VMEM] * 4,
        whole + (shape(world, 1, LANES),),
        scratch,
        fields + (spread,),
        (HBM, HBM, VMEM),
    )
    sums = lax.all_to_all(spread, AXES, 0, 0)
    older, newer, moments = call(
        functools.partial(after_kernel, rows, vecs, cols),
        "after",
        6,
        [VMEM] * 4 + [HBM] * 2,
        whole + (shape(1, SUMS),),
        scratch,
        (sums,) + fields + (older, newer),
        (HBM, HBM, VMEM),
        {4: 0, 5: 1},
    )
    return older, newer, moments[0]


def solution(mesh):
    return jax.shard_map(
        body,
        mesh=mesh,
        in_specs=(P("grp", "row", "col"), P("row", "col")),
        out_specs=(P("grp", "row", "col"), P("grp", "row", "col"), P()),
        check_vma=False,
    )
```

```python
import functools

import jax
import jax.numpy as jnp
from jax import lax
from jax.experimental import pallas as pl
from jax.experimental.pallas import tpu as pltpu
from jax.sharding import PartitionSpec as P

STEPS = 8
SCALE = 4.6
RIM_R = (STEPS + 1) // 2
RIM_C = STEPS
LANES = 128
AXES = ("grp", "row", "col")
SUMS = 2 * STEPS + 1

VMEM = pl.BlockSpec(memory_space=pltpu.VMEM)
HBM = pl.BlockSpec(memory_space=pltpu.HBM)
F32 = jnp.float32


def pack_kernel(vec, dis, top, bot, sem):
    vecs, rows, _ = vec.shape
    copies = []
    for k, (out, first) in enumerate(((top, 0), (bot, rows - RIM_R))):
        place = pl.ds(first, RIM_R)
        for part in range(4):
            some = pl.ds(part * vecs // 4, vecs // 4)
            copies.append(pltpu.make_async_copy(vec.at[some, place, :], out.at[some], sem.at[k, part]))
        copies.append(pltpu.make_async_copy(dis.at[place, :], out.at[vecs], sem.at[k, 4]))
    for copy in copies:
        copy.start()
    for copy in copies:
        copy.wait()


def load_kernel(after, vec, dis, vec_out, dis_out, sem):
    copies = [
        pltpu.make_async_copy(vec, vec_out, sem.at[0]),
        pltpu.make_async_copy(dis, dis_out, sem.at[1]),
    ]
    for copy in copies:
        copy.start()
    for copy in copies:
        copy.wait()


def turn_kernel(lo, hi, vec, dis, field, edges, dis_turned):
    vecs, rows, cols = vec.shape
    groups = LANES // vecs
    padded = rows + 2 * RIM_R
    depth = padded // groups

    def lines(p, c):
        if p < RIM_R:
            return lo[:vecs, p, c : c + LANES]
        if p < RIM_R + rows:
            return vec[:, p - RIM_R, c : c + LANES]
        return hi[:vecs, p - RIM_R - rows, c : c + LANES]

    ends = ((0, 0), (cols - LANES, LANES - RIM_C))
    for c in range(0, cols, LANES):
        for m in range(depth):
            turned = jnp.concatenate([lines(g * depth + m, c) for g in range(groups)], axis=0).T
            field[m, 8 + c : 8 + c + LANES, :] = turned
            for side, (place, first) in enumerate(ends):
                if c == place:
                    edges[side, m * RIM_C : (m + 1) * RIM_C, :] = turned[first : first + RIM_C]
        block = [
            lo[vecs, :, c : c + LANES],
            dis[:, c : c + LANES],
            hi[vecs, :, c : c + LANES],
            jnp.zeros((LANES - padded, LANES), F32),
        ]
        turned = jnp.concatenate(block, axis=0).T * (2.0 / SCALE)
        dis_turned[c : c + LANES, :] = turned
        for side, (place, first) in enumerate(ends):
            if c == place:
                edges[side, depth * RIM_C :, :] = turned[first : first + RIM_C]


def spread_rows(tile, m, vecs, depth):
    index = lax.broadcasted_iota(jnp.int32, (8, LANES), 1) // vecs * depth + m
    return jnp.take_along_axis(tile, index, axis=1)


def advance(depth, vecs, now, then, out, energy, tiles, counted, sums):
    odd = lax.broadcasted_iota(jnp.int32, (8, LANES), 0) % 2 == 1
    for t in tiles:
        here = [now(m, t, 0) for m in range(depth)]
        over = pltpu.roll(here[depth - 1], vecs, 1)
        under = pltpu.roll(here[0], LANES - vecs, 1)
        for m in range(depth):
            above = here[m - 1] if m > 0 else over
            below = here[m + 1] if m < depth - 1 else under
            vertical = jnp.where(odd, below, above) if m % 2 else jnp.where(odd, above, below)
            near = (now(m, t, -1) + now(m, t, 1)) + vertical
            latest = energy(m, t) * here[m] - (2.0 / SCALE) * near
            latest = 0.5 * latest if then is None else latest - then(m, t, 0)
            out(m, t, latest)
            if t in counted:
                sums["s"][m] = sums["s"][m] + latest * latest
                sums["r"][m] = sums["r"][m] + latest * here[m]
                if then is None:
                    sums["0"][m] = sums["0"][m] + here[m] * here[m]


def fresh(depth):
    zero = jnp.zeros((8, LANES), F32)
    return {name: [zero] * depth for name in "sr0"}


def own(parts, rows, vecs):
    depth = len(parts)
    group = lax.broadcasted_iota(jnp.int32, (8, LANES), 1) // vecs
    total = jnp.zeros((8, LANES), F32)
    for m in range(depth):
        place = group * depth + m
        kept = (place >= RIM_R) & (place < RIM_R + rows)
        total = total + jnp.where(kept, parts[m], 0.0)
    return total


def chain(field, odd, even):
    result = [(field, None, odd), (odd, field, even)]
    for n in range(2, STEPS):
        now, other = (odd, even) if n % 2 else (even, odd)
        result.append((now, other, other))
    return result


def inner_kernel(rows, vecs, cols, field, dis_turned, odd, even, partial, ene):
    depth = field.shape[0]
    tiles = cols // 8
    for t in range(tiles):
        tile = dis_turned[8 * t : 8 * t + 8, :]
        for m in range(depth):
            ene[m, 8 * t : 8 * t + 8, :] = spread_rows(tile, m, vecs, depth)

    def reader(ref):
        return lambda m, t, by: ref[m, 8 + 8 * t + by : 16 + 8 * t + by, :]

    def writer(ref):
        def write(m, t, value):
            ref[m, 8 + 8 * t : 16 + 8 * t, :] = value

        return write

    for n, (now, then, out) in enumerate(chain(field, odd, even)):
        sums = fresh(depth)
        advance(
            depth,
            vecs,
            reader(now),
            None if then is None else reader(then),
            writer(out),
            lambda m, t: ene[m, 8 * t : 8 * t + 8, :],
            range(tiles),
            range(1, tiles - 1),
            sums,
        )
        if n == 0:
            partial[0] = own(sums["0"], rows, vecs)
        partial[2 * n + 1] = own(sums["r"], rows, vecs)
        partial[2 * n + 2] = own(sums["s"], rows, vecs)


def edge_kernel(
    rows, vecs, cols, places, sites, field, dis_turned, left, right, partial, ends, spread, start, odd, even, ene
):
    depth = field.shape[0]
    at = depth * RIM_C
    for side, rim, rim_at, mine in ((0, left, 0, (0, 1)), (1, right, 2, (cols // 8 - 2, cols // 8 - 1))):
        order = [None, *mine] if rim_at == 0 else [*mine, None]
        for k, t in enumerate(order):
            if t is None:
                tile = rim[places[side], at : at + 8, :]
            else:
                tile = dis_turned[8 * t : 8 * t + 8, :]
            for m in range(depth):
                if t is None:
                    value = rim[places[side], m * RIM_C : (m + 1) * RIM_C, :]
                else:
                    value = field[m, 8 + 8 * t : 16 + 8 * t, :]
                start[side, m, 8 + 8 * k : 16 + 8 * k, :] = value
                ene[side, m, 8 * k : 8 * k + 8, :] = spread_rows(tile, m, vecs, depth)

    def reader(ref):
        return lambda m, t, by: ref[t[0], m, 8 + 8 * t[1] + by : 16 + 8 * t[1] + by, :]

    def writer(ref):
        def write(m, t, value):
            ref[t[0], m, 8 + 8 * t[1] : 16 + 8 * t[1], :] = value

        return write

    middle = ((0, 1), (1, 1))
    every = [(side, k) for side in (0, 1) for k in (0, 1, 2)]
    lane = lax.broadcasted_iota(jnp.int32, (8, LANES), 1)
    total = jnp.zeros((8, LANES), F32)
    first = []

    def place(total, k, parts):
        value = jnp.sum(partial[k] + own(parts, rows, vecs), axis=1, keepdims=True)
        if k < 2:
            first.append(jnp.sum(value, axis=0, keepdims=True))
        return total + jnp.where(lane == k, value, 0.0)

    for n, (now, then, out) in enumerate(chain(start, odd, even)):
        sums = fresh(depth)
        advance(
            depth,
            vecs,
            reader(now),
            None if then is None else reader(then),
            writer(out),
            lambda m, t: ene[t[0], m, 8 * t[1] : 8 * t[1] + 8, :],
            every if n < STEPS - 1 else middle,
            middle,
            sums,
        )
        if n == 0:
            total = place(total, 0, sums["0"])
        total = place(total, 2 * n + 1, sums["r"]) if n < STEPS else total
        total = place(total, 2 * n + 2, sums["s"])
    line = lane[:1]
    values = jnp.sum(total, axis=0, keepdims=True)
    base = jnp.where(line % 2 == 0, first[0], first[1])
    values = jnp.where(line < 2, values, 2.0 * values - base) * (1.0 / sites)
    spread[...] = jnp.broadcast_to(values[None], spread.shape)
    for k, ref in ((0, odd if STEPS % 2 == 0 else even), (1, even if STEPS % 2 == 0 else odd)):
        for side in (0, 1):
            for m in range(depth):
                ends[k, side, m] = ref[side, m, 16:24, :]


def on_first_chip():
    return (lax.axis_index("grp") == 0) & (lax.axis_index("row") < 2) & (lax.axis_index("col") == 0)


def unturn(rows, vecs, cols, prev, last, ends, prev_out, last_out, flat, sem):
    depth = prev.shape[0]
    groups = LANES // vecs
    copies = []
    for k, (ref, out) in enumerate(((prev, prev_out), (last, last_out))):
        for m in range(depth):
            for c in range(0, cols, LANES):
                low, high = 8 + c, 8 + c + LANES
                block = []
                if c == 0:
                    block.append(ends[k, 0, m])
                    low += 8
                if c == cols - LANES:
                    high -= 8
                block.append(ref[m, low:high, :])
                if c == cols - LANES:
                    block.append(ends[k, 1, m])
                turned = jnp.concatenate(block, axis=0).T
                for g in range(groups):
                    r = g * depth + m - RIM_R
                    if 0 <= r < rows:
                        flat[k, :, r, c : c + LANES] = turned[g * vecs : (g + 1) * vecs]
        copy = pltpu.make_async_copy(flat.at[k], out, sem.at[k])
        copy.start()
        copies.append(copy)
    for copy in copies:
        copy.wait()


def before_kernel(rows, vecs, cols, prev, last, ends, spread, prev_out, last_out, spread_out, flat, sem):
    spread_out[...] = spread[...]

    @pl.when(on_first_chip())
    def _():
        unturn(rows, vecs, cols, prev, last, ends, prev_out, last_out, flat, sem)


def after_kernel(rows, vecs, cols, sums, prev, last, ends, prev_in, last_in, prev_out, last_out, moments, flat, sem):
    moments[...] = jnp.sum(sums[...], axis=0)[:, :SUMS]

    @pl.when(jnp.logical_not(on_first_chip()))
    def _():
        unturn(rows, vecs, cols, prev, last, ends, prev_out, last_out, flat, sem)


def shift(array, axis, by):
    count = lax.axis_size(axis)
    return lax.ppermute(array, axis, [(i, (i + by) % count) for i in range(count)])


def shape(*dims):
    return jax.ShapeDtypeStruct(dims, F32)


def call(kernel, name, limit, ins, outs, scratch, args, out_specs=None, aliases={}):
    return pl.pallas_call(
        kernel,
        out_shape=outs,
        in_specs=ins,
        out_specs=(VMEM,) * len(outs) if out_specs is None else out_specs,
        scratch_shapes=scratch,
        input_output_aliases=aliases,
        compiler_params=pltpu.CompilerParams(vmem_limit_bytes=limit << 20),
        name=name,
    )(*args)


def body(vectors, disorder):
    vecs, rows, cols = vectors.shape
    groups = LANES // vecs
    padded = rows + 2 * RIM_R
    depth = padded // groups
    assert vecs * groups == LANES and depth * groups == padded and depth % 2 == 0
    assert rows % 8 == 0 and rows >= 2 * RIM_R and cols % LANES == 0 and cols > 2 * RIM_C
    sites, world = vecs * rows * cols, 1
    for axis in AXES:
        sites *= lax.axis_size(axis)
        world *= lax.axis_size(axis)
    dma = pltpu.SemaphoreType.DMA

    rim = shape(vecs + 1, RIM_R, cols)
    inputs = (
        pltpu.with_memory_space_constraint(vectors, pltpu.HBM),
        pltpu.with_memory_space_constraint(disorder, pltpu.HBM),
    )
    top, bot = call(pack_kernel, "pack", 2, [HBM, HBM], (rim, rim), [dma((2, 5))], inputs)
    vec, dis = call(
        load_kernel,
        "load",
        2,
        [VMEM, HBM, HBM],
        (shape(*vectors.shape), shape(*disorder.shape)),
        [dma((2,))],
        (top,) + inputs,
    )
    lo = shift(bot, "row", 1)
    hi = shift(top, "row", -1)
    wide = cols + 16
    tall = shape(depth, wide, LANES)
    field, edges, dis_turned = call(
        turn_kernel,
        "turn",
        6,
        [VMEM] * 4,
        (tall, shape(2, depth * RIM_C + 8, LANES), shape(cols, LANES)),
        [],
        (lo, hi, vec, dis),
    )
    if lax.axis_size("col") == 2:
        left = right = shift(edges, "col", 1)
        places = (1, 0)
    else:
        left, right = shift(edges[1:], "col", 1), shift(edges[:1], "col", -1)
        places = (0, 0)
    odd, even, partial = call(
        functools.partial(inner_kernel, rows, vecs, cols),
        "inner",
        8,
        [VMEM] * 2,
        (tall, tall, shape(SUMS, 8, LANES)),
        [pltpu.VMEM((depth, cols + 8, LANES), F32)],
        (field, dis_turned),
    )
    strip = pltpu.VMEM((2, depth, 40, LANES), F32)
    ends, spread = call(
        functools.partial(edge_kernel, rows, vecs, cols, places, float(sites)),
        "edge",
        6,
        [VMEM] * 5,
        (shape(2, 2, depth, 8, LANES), shape(world, 1, LANES)),
        [strip, strip, strip, pltpu.VMEM((2, depth, 24, LANES), F32)],
        (field, dis_turned, left, right, partial),
    )
    fields = ((odd, even) if STEPS % 2 == 0 else (even, odd)) + (ends,)
    whole = (shape(*vectors.shape),) * 2
    scratch = [pltpu.VMEM((2, vecs, rows, cols), F32), dma((2,))]
    older, newer, spread = call(
        functools.partial(before_kernel, rows, vecs, cols),
        "before",
        6,
        [VMEM] * 4,
        whole + (shape(world, 1, LANES),),
        scratch,
        fields + (spread,),
        (HBM, HBM, VMEM),
    )
    sums = lax.all_to_all(spread, AXES, 0, 0)
    older, newer, moments = call(
        functools.partial(after_kernel, rows, vecs, cols),
        "after",
        6,
        [VMEM] * 4 + [HBM] * 2,
        whole + (shape(1, SUMS),),
        scratch,
        (sums,) + fields + (older, newer),
        (HBM, HBM, VMEM),
        {4: 0, 5: 1},
    )
    return older, newer, moments[0]


def solution(mesh):
    return jax.shard_map(
        body,
        mesh=mesh,
        in_specs=(P("grp", "row", "col"), P("row", "col")),
        out_specs=(P("grp", "row", "col"), P("grp", "row", "col"), P()),
        check_vma=False,
    )
```

```python
import functools

import jax
import jax.numpy as jnp
from jax import lax
from jax.experimental import pallas as pl
from jax.experimental.pallas import tpu as pltpu
from jax.sharding import PartitionSpec as P

STEPS = 8
SCALE = 4.6
RIM_R = (STEPS + 1) // 2
RIM_C = STEPS
LANES = 128
AXES = ("grp", "row", "col")
SUMS = 2 * STEPS + 1

VMEM = pl.BlockSpec(memory_space=pltpu.VMEM)
HBM = pl.BlockSpec(memory_space=pltpu.HBM)
F32 = jnp.float32


def pack_kernel(vec, dis, top, bot, sem):
    vecs, rows, _ = vec.shape
    copies = []
    for k, (out, first) in enumerate(((top, 0), (bot, rows - RIM_R))):
        place = pl.ds(first, RIM_R)
        for part in range(4):
            some = pl.ds(part * vecs // 4, vecs // 4)
            copies.append(pltpu.make_async_copy(vec.at[some, place, :], out.at[some], sem.at[k, part]))
        copies.append(pltpu.make_async_copy(dis.at[place, :], out.at[vecs], sem.at[k, 4]))
    for copy in copies:
        copy.start()
    for copy in copies:
        copy.wait()


def load_kernel(after, vec, dis, vec_out, dis_out, sem):
    copies = [
        pltpu.make_async_copy(vec, vec_out, sem.at[0]),
        pltpu.make_async_copy(dis, dis_out, sem.at[1]),
    ]
    for copy in copies:
        copy.start()
    for copy in copies:
        copy.wait()


def turn_kernel(lo, hi, vec, dis, field, edges, dis_turned):
    vecs, rows, cols = vec.shape
    groups = LANES // vecs
    padded = rows + 2 * RIM_R
    depth = padded // groups

    def lines(p, c):
        if p < RIM_R:
            return lo[:vecs, p, c : c + LANES]
        if p < RIM_R + rows:
            return vec[:, p - RIM_R, c : c + LANES]
        return hi[:vecs, p - RIM_R - rows, c : c + LANES]

    ends = ((0, 0), (cols - LANES, LANES - RIM_C))
    for c in range(0, cols, LANES):
        for m in range(depth):
            turned = jnp.concatenate([lines(g * depth + m, c) for g in range(groups)], axis=0).T
            field[m, 8 + c : 8 + c + LANES, :] = turned
            for side, (place, first) in enumerate(ends):
                if c == place:
                    edges[side, m * RIM_C : (m + 1) * RIM_C, :] = turned[first : first + RIM_C]
        block = [
            lo[vecs, :, c : c + LANES],
            dis[:, c : c + LANES],
            hi[vecs, :, c : c + LANES],
            jnp.zeros((LANES - padded, LANES), F32),
        ]
        turned = jnp.concatenate(block, axis=0).T * (2.0 / SCALE)
        dis_turned[c : c + LANES, :] = turned
        for side, (place, first) in enumerate(ends):
            if c == place:
                edges[side, depth * RIM_C :, :] = turned[first : first + RIM_C]


def spread_rows(tile, m, vecs, depth):
    index = lax.broadcasted_iota(jnp.int32, (8, LANES), 1) // vecs * depth + m
    if m < 0:
        index = jnp.maximum(index, 0)
    return jnp.take_along_axis(tile, index, axis=1)


def advance(depth, vecs, now, then, out, energy, tiles, counted, sums):
    odd = lax.broadcasted_iota(jnp.int32, (8, LANES), 0) % 2 == 1
    for t in tiles:
        here = [now(m, t, 0) for m in range(depth)]
        over = pltpu.roll(here[depth - 1], vecs, 1)
        under = pltpu.roll(here[0], LANES - vecs, 1)
        for m in range(depth):
            above = here[m - 1] if m > 0 else over
            below = here[m + 1] if m < depth - 1 else under
            vertical = jnp.where(odd, below, above) if m % 2 else jnp.where(odd, above, below)
            near = (now(m, t, -1) + now(m, t, 1)) + vertical
            latest = energy(m, t) * here[m] - (2.0 / SCALE) * near
            latest = 0.5 * latest if then is None else latest - then(m, t, 0)
            out(m, t, latest)
            if t in counted:
                sums["s"][m] = sums["s"][m] + latest * latest
                sums["r"][m] = sums["r"][m] + latest * here[m]
                if then is None:
                    sums["0"][m] = sums["0"][m] + here[m] * here[m]


def fresh(depth):
    zero = jnp.zeros((8, LANES), F32)
    return {name: [zero] * depth for name in "sr0"}


def own(parts, rows, vecs):
    depth = len(parts)
    group = lax.broadcasted_iota(jnp.int32, (8, LANES), 1) // vecs
    total = jnp.zeros((8, LANES), F32)
    for m in range(depth):
        place = group * depth + m
        kept = (place >= RIM_R) & (place < RIM_R + rows)
        total = total + jnp.where(kept, parts[m], 0.0)
    return total


def chain(field, odd, even):
    result = [(field, None, odd), (odd, field, even)]
    for n in range(2, STEPS):
        now, other = (odd, even) if n % 2 else (even, odd)
        result.append((now, other, other))
    return result


def inner_kernel(rows, vecs, cols, field, dis_turned, odd, even, partial, ene):
    depth = field.shape[0]
    tiles = cols // 8
    for t in range(tiles):
        tile = dis_turned[8 * t : 8 * t + 8, :]
        for m in range(depth):
            ene[m, 8 * t : 8 * t + 8, :] = spread_rows(tile, m, vecs, depth)

    def reader(ref):
        return lambda m, t, by: ref[m, 8 + 8 * t + by : 16 + 8 * t + by, :]

    def writer(ref):
        def write(m, t, value):
            ref[m, 8 + 8 * t : 16 + 8 * t, :] = value

        return write

    for n, (now, then, out) in enumerate(chain(field, odd, even)):
        sums = fresh(depth)
        advance(
            depth,
            vecs,
            reader(now),
            None if then is None else reader(then),
            writer(out),
            lambda m, t: ene[m, 8 * t : 8 * t + 8, :],
            range(tiles),
            range(1, tiles - 1),
            sums,
        )
        if n == 0:
            partial[0] = own(sums["0"], rows, vecs)
        partial[2 * n + 1] = own(sums["r"], rows, vecs)
        partial[2 * n + 2] = own(sums["s"], rows, vecs)


def edge_kernel(
    rows, vecs, cols, places, sites, field, dis_turned, left, right, partial, ends, spread, start, odd, even, ene
):
    depth = field.shape[0]
    at = depth * RIM_C
    around = range(-1, depth + 1)
    for side, rim, rim_at, mine in ((0, left, 0, (0, 1)), (1, right, 2, (cols // 8 - 2, cols // 8 - 1))):
        order = [None, *mine] if rim_at == 0 else [*mine, None]
        for k, t in enumerate(order):
            if t is None:
                tile = rim[places[side], at : at + 8, :]
            else:
                tile = dis_turned[8 * t : 8 * t + 8, :]
            for m in range(depth):
                if t is None:
                    value = rim[places[side], m * RIM_C : (m + 1) * RIM_C, :]
                else:
                    value = field[m, 8 + 8 * t : 16 + 8 * t, :]
                start[side, m + 1, 8 + 8 * k : 16 + 8 * k, :] = value
                if m == 0:
                    start[side, depth + 1, 8 + 8 * k : 16 + 8 * k, :] = pltpu.roll(value, LANES - vecs, 1)
                if m == depth - 1:
                    start[side, 0, 8 + 8 * k : 16 + 8 * k, :] = pltpu.roll(value, vecs, 1)
            for m in around:
                ene[side, m + 1, 8 * k : 8 * k + 8, :] = spread_rows(tile, m, vecs, depth)

    middle = ((0, 1), (1, 1))
    every = [(side, k) for side in (0, 1) for k in (0, 1, 2)]
    odd_line = lax.broadcasted_iota(jnp.int32, (8, LANES), 0) % 2 == 1
    lane = lax.broadcasted_iota(jnp.int32, (8, LANES), 1)
    zero = jnp.zeros((8, LANES), F32)
    total = zero
    first = []

    def place(total, k, parts):
        value = jnp.sum(partial[k] + own(parts, rows, vecs), axis=1, keepdims=True)
        if k < 2:
            first.append(jnp.sum(value, axis=0, keepdims=True))
        return total + jnp.where(lane == k, value, 0.0)

    for n, (now, then, out) in enumerate(chain(start, odd, even)):
        squares, crosses, begin = [zero] * depth, [zero] * depth, [zero] * depth
        for side, k in every if n < STEPS - 1 else middle:
            low, high = 8 + 8 * k, 16 + 8 * k
            here = {m: now[side, m + 1, low:high, :] for m in around}
            for m in around if n % 2 == 0 else range(depth):
                above, below = here.get(m - 1, here[m]), here.get(m + 1, here[m])
                vertical = jnp.where(odd_line, below, above) if m % 2 else jnp.where(odd_line, above, below)
                near = (now[side, m + 1, low - 1 : high - 1, :] + now[side, m + 1, low + 1 : high + 1, :]) + vertical
                latest = ene[side, m + 1, 8 * k : 8 * k + 8, :] * here[m] - (2.0 / SCALE) * near
                latest = 0.5 * latest if then is None else latest - then[side, m + 1, low:high, :]
                out[side, m + 1, low:high, :] = latest
                if n % 2 == 1 and n < STEPS - 1 and m == 0:
                    out[side, depth + 1, low:high, :] = pltpu.roll(latest, LANES - vecs, 1)
                if n % 2 == 1 and n < STEPS - 1 and m == depth - 1:
                    out[side, 0, low:high, :] = pltpu.roll(latest, vecs, 1)
                if (side, k) in middle and 0 <= m < depth:
                    squares[m] = squares[m] + latest * latest
                    crosses[m] = crosses[m] + latest * here[m]
                    if n == 0:
                        begin[m] = begin[m] + here[m] * here[m]
        if n == 0:
            total = place(total, 0, begin)
        total = place(total, 2 * n + 1, crosses)
        total = place(total, 2 * n + 2, squares)
    line = lane[:1]
    values = jnp.sum(total, axis=0, keepdims=True)
    base = jnp.where(line % 2 == 0, first[0], first[1])
    values = jnp.where(line < 2, values, 2.0 * values - base) * (1.0 / sites)
    spread[...] = jnp.broadcast_to(values[None], spread.shape)
    for k, ref in ((0, odd if STEPS % 2 == 0 else even), (1, even if STEPS % 2 == 0 else odd)):
        for side in (0, 1):
            for m in range(depth):
                ends[k, side, m] = ref[side, m + 1, 16:24, :]


def on_first_chip():
    return (lax.axis_index("grp") == 0) & (lax.axis_index("row") < 2) & (lax.axis_index("col") == 0)


def unturn(rows, vecs, cols, prev, last, ends, prev_out, last_out, flat, sem):
    depth = prev.shape[0]
    groups = LANES // vecs
    copies = []
    for k, (ref, out) in enumerate(((prev, prev_out), (last, last_out))):
        for m in range(depth):
            for c in range(0, cols, LANES):
                low, high = 8 + c, 8 + c + LANES
                block = []
                if c == 0:
                    block.append(ends[k, 0, m])
                    low += 8
                if c == cols - LANES:
                    high -= 8
                block.append(ref[m, low:high, :])
                if c == cols - LANES:
                    block.append(ends[k, 1, m])
                turned = jnp.concatenate(block, axis=0).T
                for g in range(groups):
                    r = g * depth + m - RIM_R
                    if 0 <= r < rows:
                        flat[k, :, r, c : c + LANES] = turned[g * vecs : (g + 1) * vecs]
        copy = pltpu.make_async_copy(flat.at[k], out, sem.at[k])
        copy.start()
        copies.append(copy)
    for copy in copies:
        copy.wait()


def before_kernel(rows, vecs, cols, prev, last, ends, spread, prev_out, last_out, spread_out, flat, sem):
    spread_out[...] = spread[...]

    @pl.when(on_first_chip())
    def _():
        unturn(rows, vecs, cols, prev, last, ends, prev_out, last_out, flat, sem)


def after_kernel(rows, vecs, cols, sums, prev, last, ends, prev_in, last_in, prev_out, last_out, moments, flat, sem):
    moments[...] = jnp.sum(sums[...], axis=0)[:, :SUMS]

    @pl.when(jnp.logical_not(on_first_chip()))
    def _():
        unturn(rows, vecs, cols, prev, last, ends, prev_out, last_out, flat, sem)


def shift(array, axis, by):
    count = lax.axis_size(axis)
    return lax.ppermute(array, axis, [(i, (i + by) % count) for i in range(count)])


def shape(*dims):
    return jax.ShapeDtypeStruct(dims, F32)


def call(kernel, name, limit, ins, outs, scratch, args, out_specs=None, aliases={}):
    return pl.pallas_call(
        kernel,
        out_shape=outs,
        in_specs=ins,
        out_specs=(VMEM,) * len(outs) if out_specs is None else out_specs,
        scratch_shapes=scratch,
        input_output_aliases=aliases,
        compiler_params=pltpu.CompilerParams(vmem_limit_bytes=limit << 20),
        name=name,
    )(*args)


def body(vectors, disorder):
    vecs, rows, cols = vectors.shape
    groups = LANES // vecs
    padded = rows + 2 * RIM_R
    depth = padded // groups
    assert vecs * groups == LANES and depth * groups == padded and depth % 2 == 0
    assert rows % 8 == 0 and rows >= 2 * RIM_R and cols % LANES == 0 and cols > 2 * RIM_C
    sites, world = vecs * rows * cols, 1
    for axis in AXES:
        sites *= lax.axis_size(axis)
        world *= lax.axis_size(axis)
    dma = pltpu.SemaphoreType.DMA

    rim = shape(vecs + 1, RIM_R, cols)
    inputs = (
        pltpu.with_memory_space_constraint(vectors, pltpu.HBM),
        pltpu.with_memory_space_constraint(disorder, pltpu.HBM),
    )
    top, bot = call(pack_kernel, "pack", 2, [HBM, HBM], (rim, rim), [dma((2, 5))], inputs)
    vec, dis = call(
        load_kernel,
        "load",
        2,
        [VMEM, HBM, HBM],
        (shape(*vectors.shape), shape(*disorder.shape)),
        [dma((2,))],
        (top,) + inputs,
    )
    lo = shift(bot, "row", 1)
    hi = shift(top, "row", -1)
    wide = cols + 16
    tall = shape(depth, wide, LANES)
    field, edges, dis_turned = call(
        turn_kernel,
        "turn",
        6,
        [VMEM] * 4,
        (tall, shape(2, depth * RIM_C + 8, LANES), shape(cols, LANES)),
        [],
        (lo, hi, vec, dis),
    )
    if lax.axis_size("col") == 2:
        left = right = shift(edges, "col", 1)
        places = (1, 0)
    else:
        left, right = shift(edges[1:], "col", 1), shift(edges[:1], "col", -1)
        places = (0, 0)
    odd, even, partial = call(
        functools.partial(inner_kernel, rows, vecs, cols),
        "inner",
        8,
        [VMEM] * 2,
        (tall, tall, shape(SUMS, 8, LANES)),
        [pltpu.VMEM((depth, cols + 8, LANES), F32)],
        (field, dis_turned),
    )
    strip = pltpu.VMEM((2, depth + 2, 48, LANES), F32)
    ends, spread = call(
        functools.partial(edge_kernel, rows, vecs, cols, places, float(sites)),
        "edge",
        6,
        [VMEM] * 5,
        (shape(2, 2, depth, 8, LANES), shape(world, 1, LANES)),
        [strip, strip, strip, pltpu.VMEM((2, depth + 2, 24, LANES), F32)],
        (field, dis_turned, left, right, partial),
    )
    fields = ((odd, even) if STEPS % 2 == 0 else (even, odd)) + (ends,)
    whole = (shape(*vectors.shape),) * 2
    scratch = [pltpu.VMEM((2, vecs, rows, cols), F32), dma((2,))]
    older, newer, spread = call(
        functools.partial(before_kernel, rows, vecs, cols),
        "before",
        6,
        [VMEM] * 4,
        whole + (shape(world, 1, LANES),),
        scratch,
        fields + (spread,),
        (HBM, HBM, VMEM),
    )
    sums = lax.all_to_all(spread, AXES, 0, 0)
    older, newer, moments = call(
        functools.partial(after_kernel, rows, vecs, cols),
        "after",
        6,
        [VMEM] * 4 + [HBM] * 2,
        whole + (shape(1, SUMS),),
        scratch,
        (sums,) + fields + (older, newer),
        (HBM, HBM, VMEM),
        {4: 0, 5: 1},
    )
    return older, newer, moments[0]


def solution(mesh):
    return jax.shard_map(
        body,
        mesh=mesh,
        in_specs=(P("grp", "row", "col"), P("row", "col")),
        out_specs=(P("grp", "row", "col"), P("grp", "row", "col"), P()),
        check_vma=False,
    )
```
